32 devices in a mesh: copy: 4 (over y, x), fsdp: 2 (over core), cols: 4 (over z).
Axes of the slice: x: 2, y: 2, z: 4, core: 2. Of those that a mesh axis runs over, the one named last changes fastest.
Arguments:
- train_gate: float32 [8192, 8192], P(('copy', 'fsdp'), 'cols'), parts along dimension 0, may hold values from -0.1875 to 0.1875
- drift_gate: float32 [8192, 8192], P(('copy', 'fsdp'), 'cols'), parts along dimension 0, may hold values from -6 to 6
- spread_gate: float32 [8192, 8192], P(('copy', 'fsdp'), 'cols'), parts along dimension 0, may hold values from 0.1 to 10
- train_up: float32 [8192, 8192], P(('copy', 'fsdp'), 'cols'), parts along dimension 0, may hold values from -0.1875 to 0.1875
- drift_up: float32 [8192, 8192], P(('copy', 'fsdp'), 'cols'), parts along dimension 0, may hold values from -6 to 6
- spread_up: float32 [8192, 8192], P(('copy', 'fsdp'), 'cols'), parts along dimension 0, may hold values from 0.1 to 10
- norm_train: float32 [8192], P(('copy', 'fsdp', 'cols')), parts along dimension 0, may hold values from 0.25 to 1.75
- norm_step: float32 [8192], P(('copy', 'fsdp', 'cols')), parts along dimension 0, may hold values from -0.3 to 0.3
Outputs:
- serve_gate: bfloat16 [8192, 8192], P('copy', 'cols'), parts along dimension 0
- serve_up: bfloat16 [8192, 8192], P('copy', 'cols'), parts along dimension 0
- scale_gate: float32 [32768], P(('copy', 'cols')), parts along dimension 0
- scale_up: float32 [32768], P(('copy', 'cols')), parts along dimension 0
- serve_norm: bfloat16 [8192], P('copy'), parts along dimension 0
- fresh_gate: float32 [8192, 8192], P(('copy', 'fsdp'), 'cols'), parts along dimension 0
- fresh_up: float32 [8192, 8192], P(('copy', 'fsdp'), 'cols'), parts along dimension 0
The draws below stay inside these ranges and needn't reach their ends.
There are 4 independent parts, one for each index of `copy`. The reference program is written for one: setup_inputs(seed, part) draws one part's arguments, and reference() takes and returns one part's arrays. A program takes and returns all parts, laid end to end along the dimension named above; each array names one. Nothing has to cross between parts.
All inputs are finite; a program needn't handle non-finite values.
Results may differ from the reference program's by a relative error of at most 0.001.
Values may be sent and summed in bfloat16 or wider, within the bound.
A program may use at most 192 MiB of HBM per device.

```python
import math
import jax
import jax.numpy as jnp
from jax import lax

D_MODEL = 2048
D_INNER = 8192


def with_spikes(values, key, source, target, shards_of, factor):
    def block_of(axis_at):
        return (jnp.arange(values.shape[axis_at]) // (values.shape[axis_at] // shards_of)).reshape((-1,) + (1,) * (values.ndim - 1 - axis_at))

    near = jax.random.permutation(key, shards_of)[block_of(target)]
    far = (block_of(target) + shards_of // 2) % shards_of
    return jnp.where((block_of(source) == near) | (block_of(source) == far), factor * values, values)


def level_of(stream_key, shape, shards, smallest, largest):
    factor_of, own = 1.0, jax.random.fold_in(stream_key, 6)
    for dim, parts in shards:
        steps = jnp.exp(jax.random.uniform(jax.random.fold_in(own, dim), (parts,), jnp.float32, smallest / len(shards), largest / len(shards)))
        factor_of = factor_of * jnp.repeat(steps, shape[dim] // parts).reshape([-1 if axis == dim else 1 for axis in range(len(shape))])
    return factor_of


def normal_values(rng, shape, scale, reach, pieces=(), held_as=jnp.bfloat16):
    loudness = level_of(rng, shape, pieces, -0.22, 0.18) if pieces else 1.0
    drawn = jax.random.normal(rng, shape, jnp.float32) * scale * loudness
    return jnp.minimum(jnp.maximum(drawn, -reach), reach).astype(held_as)


def gaussian_with(rng, dims, spread, reach, pieces, heavy, kind=jnp.bfloat16):
    array = spread * jax.random.normal(rng, dims, jnp.float32)
    if pieces:
        array = array * level_of(rng, dims, pieces, -0.22, 0.18)
    return jnp.clip(with_spikes(array, jax.random.fold_in(rng, 3), *heavy), -reach, reach).astype(kind)


def setup_inputs(seed: int = 0, part: int = 0) -> dict:
    streams_of = jax.random.split(jax.random.key(seed), 9)
    part_splits = jax.random.split(jax.random.fold_in(streams_of[8], part), 9)
    return {
        "train_gate": gaussian_with(part_splits[0], (D_MODEL, D_INNER), D_MODEL ** -0.5, 0.1875, ((0, 2), (1, 4)), (0, 1, 4, 2.0), jnp.float32),
        "drift_gate": normal_values(part_splits[1], (D_MODEL, D_INNER), 1.0, 6.0, ((0, 2), (1, 4)), jnp.float32),
        "spread_gate": jnp.clip(jnp.exp(math.log(10.0) - 4.6051702 * jax.random.uniform(part_splits[2], (D_MODEL, D_INNER), jnp.float32) ** level_of(part_splits[2], (D_MODEL, D_INNER), ((0, 2), (1, 4)), -0.2, 0.2)), 0.1, 10.0),
        "train_up": gaussian_with(part_splits[3], (D_MODEL, D_INNER), D_MODEL ** -0.5, 0.1875, ((0, 2), (1, 4)), (0, 1, 4, 2.0), jnp.float32),
        "drift_up": normal_values(part_splits[4], (D_MODEL, D_INNER), 1.0, 6.0, ((0, 2), (1, 4)), jnp.float32),
        "spread_up": jnp.clip(jnp.exp(math.log(10.0) - 4.6051702 * jax.random.uniform(part_splits[5], (D_MODEL, D_INNER), jnp.float32) ** level_of(part_splits[5], (D_MODEL, D_INNER), ((0, 2), (1, 4)), -0.2, 0.2)), 0.1, 10.0),
        "norm_train": jnp.clip(1.0 + 0.15 * jax.random.normal(part_splits[6], (D_MODEL,), jnp.float32), 0.25, 1.75),
        "norm_step": jnp.clip(jax.random.uniform(part_splits[7], (D_MODEL,), jnp.float32, -0.3, 0.3) * level_of(part_splits[7], (D_MODEL,), ((0, 8),), -0.4, 0.0), -0.3, 0.3),
    }


learn_rate = 0.02
decay_rate = 0.1
tiny_value = 1e-08

def reference(train_gate, drift_gate, spread_gate, train_up, drift_up, spread_up, norm_train, norm_step):
    fresh_gate = train_gate - learn_rate * (drift_gate / (jnp.sqrt(spread_gate) + tiny_value) + decay_rate * train_gate)
    fresh_up = train_up - learn_rate * (drift_up / (jnp.sqrt(spread_up) + tiny_value) + decay_rate * train_up)
    scale_gate = jnp.sqrt(lax.optimization_barrier(jnp.sum(fresh_gate * fresh_gate, axis=0)))
    serve_gate = (fresh_gate / scale_gate).astype(jnp.bfloat16)
    scale_up = jnp.sqrt(lax.optimization_barrier(jnp.sum(fresh_up * fresh_up, axis=0)))
    serve_up = (fresh_up / scale_up).astype(jnp.bfloat16)
    serve_norm = (norm_train + norm_step).astype(jnp.bfloat16)
    return (serve_gate, serve_up, scale_gate, scale_up, serve_norm, fresh_gate, fresh_up)
```

```python
import functools

import jax
import jax.numpy as jnp
from jax import lax
from jax.experimental import pallas as pl
from jax.experimental.pallas import tpu as pltpu
from jax.sharding import PartitionSpec as P

learn_rate = 0.02
decay_rate = 0.1
tiny_value = 1e-08

LANES = 128
SUBLANES = 8
SLOTS = 3
WIDTH = 256
ROWS = 32
MESH = pl.DeviceIdType.MESH


def step_kernel(sizes, *refs):
    share, across, rows, columns, width = sizes
    group = share * across
    chunks = columns // width
    steps = 2 * chunks
    sources = (refs[0:3], refs[3:6])
    norm_ref = refs[6]
    fresh_ref, serve_ref, scale_ref, norm_out = refs[7:11]
    inbox, sums, in_sem, sum_send, sum_recv, half_send, half_recv, norm_send, norm_recv = refs[11:]
    me = lax.axis_index("fsdp")
    column = lax.axis_index("cols")
    place = me * across + column

    def start_input(which, slot, index):
        offset = pl.multiple_of(index * width, width)
        for k in range(3):
            pltpu.make_async_copy(
                sources[which][k].at[:, pl.ds(offset, width)], inbox.at[slot, k], in_sem.at[slot, k]
            ).start()

    def begin(c):
        slot = lax.rem(c, SLOTS)

        @pl.when(c < chunks)
        def _():
            start_input(0, slot, c)

        @pl.when(c >= chunks)
        def _():
            start_input(1, slot, c - chunks)

    def sum_copy(c, k):
        return pltpu.make_async_remote_copy(
            src_ref=sums.at[c, me],
            dst_ref=sums.at[c, me],
            send_sem=sum_send.at[c, k - 1],
            recv_sem=sum_recv.at[c, k - 1],
            device_id={"fsdp": lax.rem(me + k, share)},
            device_id_type=MESH,
        )

    def half_copy(c, k):
        part = serve_ref.at[
            c // chunks,
            pl.ds(pl.multiple_of(me * rows, rows), rows),
            pl.ds(pl.multiple_of(lax.rem(c, chunks) * width, width), width),
        ]
        return pltpu.make_async_remote_copy(
            src_ref=part,
            dst_ref=part,
            send_sem=half_send.at[c, k - 1],
            recv_sem=half_recv.at[c, k - 1],
            device_id={"fsdp": lax.rem(me + k, share)},
            device_id_type=MESH,
        )

    def norm_copy(k):
        other = lax.rem(place + k, group)
        return pltpu.make_async_remote_copy(
            src_ref=norm_out.at[place],
            dst_ref=norm_out.at[place],
            send_sem=norm_send.at[k - 1],
            recv_sem=norm_recv.at[k - 1],
            device_id={"fsdp": other // across, "cols": lax.rem(other, across)},
            device_id_type=MESH,
        )

    for c in range(min(SLOTS, steps)):
        start_input(c // chunks, c, c % chunks)

    barrier = pltpu.get_barrier_semaphore()
    for k in range(1, group):
        other = lax.rem(place + k, group)
        pl.semaphore_signal(
            barrier,
            inc=1,
            device_id={"fsdp": other // across, "cols": lax.rem(other, across)},
            device_id_type=MESH,
        )
    norm_out[place] = norm_ref[...]
    pl.semaphore_wait(barrier, group - 1)
    for k in range(1, group):
        norm_copy(k).start()

    def compute(c):
        slot = lax.rem(c, SLOTS)
        which = c // chunks
        offset = pl.multiple_of(lax.rem(c, chunks) * width, width)
        for k in range(3):
            pltpu.make_async_copy(
                sources[0][k].at[:, pl.ds(0, width)], inbox.at[slot, k], in_sem.at[slot, k]
            ).wait()

        def block(i, total):
            at = pl.ds(pl.multiple_of(i * ROWS, ROWS), ROWS)
            train = inbox[slot, 0, at, :]
            drift = inbox[slot, 1, at, :]
            spread = inbox[slot, 2, at, :]
            root = spread * lax.rsqrt(spread)
            fresh = train * (1.0 - learn_rate * decay_rate) - learn_rate * (
                drift / (root + tiny_value)
            )
            fresh_ref[which, at, pl.ds(offset, width)] = fresh
            square = (fresh * fresh).reshape(ROWS // SUBLANES, SUBLANES, width)
            return total + jnp.sum(square, axis=0)

        sums[c, me] = lax.fori_loop(
            0, rows // ROWS, block, jnp.zeros((SUBLANES, width), jnp.float32), unroll=2
        )
        for k in range(1, share):
            sum_copy(c, k).start()

        @pl.when(c + SLOTS < steps)
        def _():
            begin(c + SLOTS)

    def narrow(c):
        which = c // chunks
        offset = pl.multiple_of(lax.rem(c, chunks) * width, width)
        for k in range(1, share):
            sum_copy(c, k).wait_recv()
        total = sums[c, 0]
        for j in range(1, share):
            total += sums[c, j]
        scale = jnp.sqrt(jnp.sum(total, axis=0, keepdims=True))
        for j in range(width // LANES):
            scale_ref[pl.ds(c * (width // LANES) + j, 1), :] = scale[:, j * LANES : (j + 1) * LANES]
        inverse = 1.0 / scale

        def block(i, carry):
            at = pl.ds(pl.multiple_of(i * ROWS, ROWS), ROWS)
            to = pl.ds(pl.multiple_of(me * rows + i * ROWS, ROWS), ROWS)
            serve_ref[which, to, pl.ds(offset, width)] = (
                fresh_ref[which, at, pl.ds(offset, width)] * inverse
            ).astype(jnp.bfloat16)
            return carry

        lax.fori_loop(0, rows // ROWS, block, 0, unroll=2)
        for k in range(1, share):
            half_copy(c, k).start()

    def step(c, carry):
        @pl.when(c < steps)
        def _():
            compute(c)

        @pl.when(c >= 1)
        def _():
            narrow(c - 1)

        return carry

    lax.fori_loop(0, steps + 1, step, 0)

    for k in range(1, group):
        norm_copy(k).wait()

    def finish(c, carry):
        for k in range(1, share):
            sum_copy(c, k).wait_send()
            half_copy(c, k).wait()
        return carry

    lax.fori_loop(0, steps, finish, 0)


def write_kernel(fresh_ref, serve_ref, scale_ref, *refs):
    outs, sem = refs[:6], refs[6]
    half = scale_ref.shape[0] // 2
    copies = [
        pltpu.make_async_copy(source, target, sem.at[n])
        for n, (source, target) in enumerate(
            zip(
                (
                    fresh_ref.at[0],
                    fresh_ref.at[1],
                    serve_ref.at[0],
                    serve_ref.at[1],
                    scale_ref.at[pl.ds(0, half)],
                    scale_ref.at[pl.ds(half, half)],
                ),
                outs,
            )
        )
    ]
    for copy in copies:
        copy.start()
    for copy in copies:
        copy.wait()


def body(share, across, train_gate, drift_gate, spread_gate, train_up, drift_up, spread_up, norm_train, norm_step):
    rows, columns = train_gate.shape
    group = share * across
    steps = 2 * columns // WIDTH
    piece = norm_train.shape[0]
    tile = SUBLANES * LANES
    padded = -(-piece // tile) * tile
    norm = jnp.pad(norm_train + norm_step, (0, padded - piece)).reshape(padded // LANES, LANES)
    big = (train_gate, drift_gate, spread_gate, train_up, drift_up, spread_up)
    vmem = pl.BlockSpec(memory_space=pltpu.VMEM)
    hbm = pl.BlockSpec(memory_space=pltpu.HBM)
    fresh, serve, scale, norms = pl.pallas_call(
        functools.partial(step_kernel, (share, across, rows, columns, WIDTH)),
        out_shape=(
            pltpu.VMEM((2, rows, columns), jnp.float32),
            pltpu.VMEM((2, share * rows, columns), jnp.bfloat16),
            pltpu.VMEM((2 * columns // LANES, LANES), jnp.float32),
            pltpu.VMEM((group, padded // LANES, LANES), jnp.float32),
        ),
        in_specs=[hbm] * 6 + [vmem],
        out_specs=(vmem,) * 4,
        scratch_shapes=[
            pltpu.VMEM((SLOTS, 3, rows, WIDTH), jnp.float32),
            pltpu.VMEM((steps, share, SUBLANES, WIDTH), jnp.float32),
            pltpu.SemaphoreType.DMA((SLOTS, 3)),
            pltpu.SemaphoreType.DMA((steps, share - 1)),
            pltpu.SemaphoreType.DMA((steps, share - 1)),
            pltpu.SemaphoreType.DMA((steps, share - 1)),
            pltpu.SemaphoreType.DMA((steps, share - 1)),
            pltpu.SemaphoreType.DMA((group - 1,)),
            pltpu.SemaphoreType.DMA((group - 1,)),
        ],
        compiler_params=pltpu.CompilerParams(
            collective_id=0, has_side_effects=True, vmem_limit_bytes=12 * 2**20
        ),
        name="step_kernel",
    )(*[pltpu.with_memory_space_constraint(x, pltpu.HBM) for x in big], norm)
    held = [pltpu.with_memory_space_constraint(x, pltpu.VMEM) for x in (fresh, serve, scale)]
    fresh_gate, fresh_up, serve_gate, serve_up, scale_gate, scale_up = pl.pallas_call(
        write_kernel,
        out_shape=(
            pltpu.HBM((rows, columns), jnp.float32),
            pltpu.HBM((rows, columns), jnp.float32),
            pltpu.HBM((share * rows, columns), jnp.bfloat16),
            pltpu.HBM((share * rows, columns), jnp.bfloat16),
            pltpu.HBM((columns // LANES, LANES), jnp.float32),
            pltpu.HBM((columns // LANES, LANES), jnp.float32),
        ),
        in_specs=[vmem] * 3,
        out_specs=(hbm,) * 6,
        scratch_shapes=[pltpu.SemaphoreType.DMA((6,))],
        compiler_params=pltpu.CompilerParams(vmem_limit_bytes=2**20),
        name="write_kernel",
    )(*held)
    serve_norm = norms.reshape(group, padded)[:, :piece].reshape(group * piece).astype(jnp.bfloat16)
    return (
        serve_gate,
        serve_up,
        scale_gate.reshape(columns),
        scale_up.reshape(columns),
        serve_norm,
        fresh_gate,
        fresh_up,
    )


def solution(mesh):
    share, across = mesh.shape["fsdp"], mesh.shape["cols"]
    weight = P(("copy", "fsdp"), "cols")
    gain = P(("copy", "fsdp", "cols"))
    return jax.shard_map(
        functools.partial(body, share, across),
        mesh=mesh,
        in_specs=(weight,) * 6 + (gain, gain),
        out_specs=(
            P("copy", "cols"),
            P("copy", "cols"),
            P(("copy", "cols")),
            P(("copy", "cols")),
            P("copy"),
            weight,
            weight,
        ),
        check_vma=False,
    )
```
